32 devices in a mesh: grp: 2 (over y), slab: 4 (over z), orb: 2 (over x), rep: 2 (over core).
Axes of the slice: x: 2, y: 2, z: 4, core: 2. Of those that a mesh axis runs over, the one named last changes fastest.
Arguments:
- orbitals: bfloat16 [16, 32, 1024], P(('grp', 'slab', 'orb')), parts along dimension 0, may hold values from -6 to 6
- corners: int32 [16, 3], P('grp'), parts along dimension 0, may hold values from 0 to 191, as said below
- partners: int32 [16, 24], P(('grp', 'slab', 'orb')), parts along dimension 0, may hold values from -1 to 7, as said below
- kernel: float32 [32, 1024], replicated, may hold values from 0.05 to 5
Outputs:
- exchange_boxes: float32 [16, 32, 1024], P(('grp', 'slab', 'orb')), parts along dimension 0
- exchange_energy: float32 [2], P('grp'), parts along dimension 0
The draws below stay inside these ranges and needn't reach their ends.
There are 2 independent parts, one for each index of `grp`. The reference program is written for one: setup_inputs(seed, part) draws one part's arguments, and reference() takes and returns one part's arrays. A program takes and returns all parts, laid end to end along the dimension named above; an argument that names none is the same for every part. Nothing has to cross between parts.
Inputs may be any that keep to these rules, and one draw needn't show every extreme that they name: corners[i, 2] lies in the slab of orbital i: from 12 * (i // (1 * 2)) to 12 more less one; corners[i, 0] and corners[i, 1] lie below 192. `partners`: row i starts with i itself, names distinct orbitals whose boxes intersect box i (every component of o is above -32 and below 32), and has its -1 entries only after all others.
All inputs are finite; a program needn't handle non-finite values.
Results may differ from the reference program's by a relative error of at most 0.0003.
Values may be sent and summed in bfloat16 or wider, within the bound.
A program may use at most 64 MiB of HBM per device.

```python
import math
import jax
import jax.numpy as jnp
from jax import lax

B = 32
G = 192
ZDEV = 12
ORB_DEV = 1
NB = 24
NORB = 8
N_SLAB = 4
N_ORB = 2


def pair_tables(key):
    orbital_count = NORB
    group_size = ORB_DEV * N_ORB
    ranked_count = min(NB, NORB)
    subkeys = jax.random.split(key, 5)
    orbital_ids = jnp.arange(orbital_count, dtype=jnp.int32)
    slab_ids = orbital_ids // group_size
    corner_x = jnp.mod(jax.random.randint(subkeys[0], (orbital_count,), -B, B), G)
    corner_y = jnp.mod(jax.random.randint(subkeys[1], (orbital_count,), -B, B), G)
    corner_z = slab_ids * ZDEV + jax.random.randint(subkeys[2], (orbital_count,), 0, ZDEV)
    corners = jnp.stack([corner_x, corner_y, corner_z], axis=1).astype(jnp.int32)
    lengths = jnp.array([G, G, ZDEV * N_SLAB], jnp.int32)
    deltas = corners[:, None, :] - corners[None, :, :]
    halfway = lengths // 2
    offsets = jnp.mod(deltas + halfway, lengths) - halfway
    intersection = jnp.all(jnp.abs(offsets) < B, axis=2)
    random_rank = jax.random.randint(subkeys[3], (orbital_count, orbital_count), 0, (1 << 29) // orbital_count)
    scores = jnp.where(intersection, 1 << 30, 0) + random_rank * orbital_count + orbital_ids[None, :]
    scores = jnp.where(orbital_ids[:, None] == orbital_ids[None, :], jnp.int32(2147483647), scores).astype(jnp.int32)
    ranked = lax.top_k(scores, ranked_count)[1].astype(jnp.int32)
    picked = jnp.take_along_axis(intersection, ranked, axis=1)
    if ranked_count < NB:
        ranked = jnp.concatenate([ranked, jnp.zeros((orbital_count, NB - ranked_count), jnp.int32)], axis=1)
        picked = jnp.concatenate([picked, jnp.zeros((orbital_count, NB - ranked_count), bool)], axis=1)
    filled = jax.random.randint(subkeys[4], (orbital_count, 1), 1, NB + 1)
    slot_ids = jnp.arange(NB, dtype=jnp.int32)[None, :]
    usable = (slot_ids < filled) & picked
    partners = jnp.where(usable, ranked, -1).astype(jnp.int32)
    return (corners, partners)


def draw_corners(key, part):
    return pair_tables(jax.random.fold_in(key, 11))[0]


def draw_partners(key, part):
    return pair_tables(jax.random.fold_in(key, 11))[1]


def levels(own_key, shape, pieces, least, high):
    factor_of, own = 1.0, jax.random.fold_in(own_key, 6)
    for position, blocks in pieces:
        steps = jnp.exp(jax.random.uniform(jax.random.fold_in(own, position), (blocks,), jnp.float32, least / len(pieces), high / len(pieces)))
        factor_of = factor_of * jnp.repeat(steps, shape[position] // blocks).reshape([-1 if axis == position else 1 for axis in range(len(shape))])
    return factor_of


def normal_values(own_key, shape, width, reach, shards=(), held_as=jnp.bfloat16):
    gain = levels(own_key, shape, shards, -0.22, 0.18) if shards else 1.0
    result = jax.random.normal(own_key, shape, jnp.float32) * width * gain
    return jnp.minimum(jnp.maximum(result, -reach), reach).astype(held_as)


def setup_inputs(seed: int = 0, part: int = 0) -> dict:
    arg_keys = jax.random.split(jax.random.key(seed), 5)
    own_keys = jax.random.split(jax.random.fold_in(arg_keys[4], part), 5)
    return {
        "orbitals": normal_values(own_keys[0], (NORB, B, B * B), 1.0, 6.0, ((0, 8),)),
        "corners": draw_corners(jax.random.fold_in(jax.random.fold_in(arg_keys[4], part), 71), part),
        "partners": draw_partners(jax.random.fold_in(jax.random.fold_in(arg_keys[4], part), 71), part),
        "kernel": jnp.clip(jnp.exp(jax.random.uniform(arg_keys[3], (B, B * B), jnp.float32, math.log(0.05), math.log(5.0))), 0.05, 5.0),
    }


def wrapped(deltas, lengths):
    halfway = lengths // 2
    return jnp.mod(deltas + halfway, lengths) - halfway


def reference(orbitals, corners, partners, kernel):
    box_edge = orbitals.shape[1]
    box_count = orbitals.shape[0]
    cube_view = orbitals.reshape(box_count, box_edge, box_edge, box_edge)
    spectrum = kernel.reshape(box_edge, box_edge, box_edge)
    lengths = jnp.array([G, G, ZDEV * N_SLAB], jnp.int32)

    def one_orbital(orbital_id):
        centre = cube_view[orbital_id].astype(jnp.float32)
        corner = corners[orbital_id]

        def single_pair(partner):
            usable = partner >= 0
            safe_id = jnp.maximum(partner, 0).astype(jnp.int32)
            offset = wrapped(corner - corners[safe_id], lengths).astype(jnp.int32)
            padded = jnp.pad(cube_view[safe_id].astype(jnp.float32), box_edge)
            anchor = (offset + box_edge).astype(jnp.int32)
            shifted = lax.dynamic_slice(padded, (anchor[0], anchor[1], anchor[2]), (box_edge, box_edge, box_edge))
            shifted = jnp.where(usable, shifted, jnp.zeros_like(shifted))
            density = centre * shifted
            potential = jnp.real(jnp.fft.ifftn(spectrum * jnp.fft.fftn(density)))
            return potential * shifted, jnp.sum(density * potential)

        pair_terms, energies = lax.map(single_pair, partners[orbital_id])
        return -jnp.sum(pair_terms, axis=0), jnp.sum(energies)

    exchange_boxes, energies = lax.map(one_orbital, jnp.arange(box_count, dtype=jnp.int32))
    exchange_energy = -jnp.sum(energies) / (2.0 * box_count * box_edge ** 3)
    return exchange_boxes.reshape(box_count, box_edge, box_edge * box_edge), exchange_energy.reshape(1)
```

```python
import functools
import math

import jax
import jax.numpy as jnp
import numpy as np
from jax import lax
from jax.experimental import pallas as pl
from jax.experimental.pallas import tpu as pltpu
from jax.sharding import PartitionSpec as P

G = 192
ZDEV = 12
RADIX = 4
FIELDS = 2
MESH = pl.DeviceIdType.MESH


def split_np(values):
    high = values.astype(jnp.bfloat16)
    low = (values - high.astype(np.float64)).astype(jnp.bfloat16)
    return high, low


@functools.lru_cache(None)
def tables(edge):
    inner = edge // RADIX
    part = inner * edge
    turn = 2.0 * math.pi / edge
    ids = np.arange(edge)
    angles = (ids[:, None] * ids[None, :] % edge) * turn
    cosine, sine = np.cos(angles), np.sin(angles)
    edge_table = np.block([[cosine, sine], [-sine, cosine]])
    high, low = split_np(edge_table)
    edge_stack = np.concatenate([high, high, low], axis=1)
    lanes = np.arange(part)
    lane_b, lane_c = lanes // edge, lanes % edge
    phases = (RADIX * lane_b[:, None] * lane_b[None, :] + lane_c[:, None] * lane_c[None, :]) % edge
    cosine, sine = np.cos(phases * turn), np.sin(phases * turn)
    blocks = []
    for half in (np.concatenate([cosine, -sine], axis=1), np.concatenate([sine, cosine], axis=1)):
        high, low = split_np(half)
        blocks += [high, high, low]
    plane_stack = np.concatenate(blocks, axis=0)
    twiddle = []
    for first in range(RADIX):
        phase = (lane_b * first % edge) * turn
        twiddle += [np.cos(phase), np.sin(phase)]
    twiddle = np.stack(twiddle).astype(np.float32)
    flips = []
    for outer in (-lane_b % inner, inner - 1 - lane_b):
        source = outer * edge + (-lane_c % edge)
        flips.append((lanes[:, None] == source[None, :]).astype(jnp.bfloat16))
    flips = np.stack(flips)
    rows = (ids[:, None] == (-ids % edge)[None, :]).astype(jnp.bfloat16)
    row_flip = np.concatenate([rows, rows], axis=1)
    return edge_stack, plane_stack, twiddle, flips, row_flip


def parts(values):
    high = values.astype(jnp.bfloat16)
    return high, (values - high.astype(jnp.float32)).astype(jnp.bfloat16)


def dot(left, right):
    return jnp.dot(left, right, preferred_element_type=jnp.float32)


def butterfly(re, im):
    sum_re, sum_im = re[0] + re[2], im[0] + im[2]
    dif_re, dif_im = re[0] - re[2], im[0] - im[2]
    odd_re, odd_im = re[1] + re[3], im[1] + im[3]
    gap_re, gap_im = re[1] - re[3], im[1] - im[3]
    return (
        [sum_re + odd_re, dif_re + gap_im, sum_re - odd_re, dif_re - gap_im],
        [sum_im + odd_im, dif_im - gap_re, sum_im - odd_im, dif_im + gap_re],
    )


def twiddled(re, im, first, twiddle):
    if first == 0:
        return re, im
    cosine, sine = twiddle[2 * first : 2 * first + 1], twiddle[2 * first + 1 : 2 * first + 2]
    return re * cosine + im * sine, im * cosine - re * sine


def plane_turn(blocks, plane_table):
    rows = []
    for re, im in blocks:
        re_high, re_low = parts(re)
        im_high, im_low = parts(im)
        rows.append(
            jnp.concatenate([re_high, re_low, re_high, im_high, im_low, im_high], axis=1)
        )
    result = dot(jnp.concatenate(rows, axis=0), plane_table)
    edge, part = blocks[0][0].shape
    return [
        (result[n * edge : (n + 1) * edge, :part], result[n * edge : (n + 1) * edge, part:])
        for n in range(len(blocks))
    ]


def edge_turn(block, edge_table):
    re, im = block
    edge = re.shape[0]
    re_high, re_low = parts(re)
    im_high, im_low = parts(im)
    column = jnp.concatenate([re_high, im_high, re_low, im_low, re_high, im_high], axis=0)
    result = dot(edge_table, column)
    return result[:edge], result[edge:]


def prepared_kernel(values, flips, row_flip, edge):
    inner = edge // RADIX
    part = inner * edge
    width = RADIX * edge
    segment = lax.broadcasted_iota(jnp.int32, (edge, width), 1) // edge
    chunks = []
    for first in range(RADIX):
        pieces = []
        for group in range(part // width):
            piece = None
            for place in range(RADIX):
                source = RADIX * group + place
                moved = values[:, source * width : (source + 1) * width]
                shift = (place - first) * edge % width
                if shift:
                    moved = pltpu.roll(moved, shift, 1)
                piece = moved if piece is None else jnp.where(segment == place, moved, piece)
            pieces.append(piece)
        chunks.append(jnp.concatenate(pieces, axis=1))
    scale = 0.5 / float(edge**3)
    result = []
    for first in range(RADIX):
        high, low = parts(chunks[-first % RADIX])
        flip = flips[0] if first == 0 else flips[1]
        swapped = dot(jnp.concatenate([high, low], axis=0), flip).astype(jnp.bfloat16)
        result.append((chunks[first] + dot(row_flip, swapped)) * scale)
    return result


def fused(
    cfg,
    partners,
    corners,
    orbital,
    kernel,
    edge_table,
    plane_hbm,
    twiddle_ref,
    flips,
    row_flip,
    mine,
    theirs,
    energy_out,
    boxes,
    plane_table,
    spectrum,
    energies,
    table_sem,
    box_send,
    box_recv,
    fwd_send,
    fwd_recv,
    out_send,
    out_recv,
    energy_send,
    energy_recv,
):
    slabs, orbs, reps, steps, shift_back, slot_count, stages = cfg
    edge, plane = orbital.shape[1], orbital.shape[2]
    slab, orb, rep = lax.axis_index("slab"), lax.axis_index("orb"), lax.axis_index("rep")
    sizes = {"slab": slabs, "orb": orbs, "rep": reps}
    here = {"slab": slab, "orb": orb, "rep": rep}

    def place(moves):
        return {a: lax.rem(here[a] + moves[a] % sizes[a], sizes[a]) for a in moves}

    box_moves = [(t, u) for t in steps for u in range(orbs) if (t % slabs, u) != (0, 0)]
    reached = {(t % slabs, u, 0) for t, u in box_moves} | {(0, 0, v) for v in range(1, reps)}
    stage_moves = []
    for axes in stages:
        moves = [{}]
        for a in axes:
            moves = [dict(m, **{a: n}) for m in moves for n in range(sizes[a])]
        stage_moves.append([m for m in moves if any(m.values())])
        reached |= {(m.get("slab", 0), m.get("orb", 0), m.get("rep", 0)) for m in stage_moves[-1]}
    reached |= {(-t % slabs, -u % orbs, -v % reps) for t, u, v in reached}
    reached = sorted(reached)

    table_copy = pltpu.make_async_copy(plane_hbm, plane_table, table_sem)
    table_copy.start()
    barrier = pltpu.get_barrier_semaphore()
    for t, u, v in reached:
        pl.semaphore_signal(
            barrier,
            inc=1,
            device_id=place({"slab": t, "orb": u, "rep": v}),
            device_id_type=MESH,
        )
    pl.semaphore_wait(barrier, len(reached))

    def slot_of(t, u):
        return (t + shift_back) % slabs * orbs + u % orbs

    cut = edge // reps
    share = pl.ds(pl.multiple_of(rep * cut, cut), cut)
    sends = []
    for t, u in box_moves:
        target = slot_of(-t, -u)
        copy = pltpu.make_async_remote_copy(
            src_ref=orbital.at[0, share],
            dst_ref=boxes.at[target, share],
            send_sem=box_send.at[target],
            recv_sem=box_recv.at[target],
            device_id=place({"slab": t, "orb": u}),
            device_id_type=MESH,
        )
        copy.start()
        sends.append((slot_of(t, u), copy))

    centre = orbital[0].astype(jnp.float32)
    boxes[slot_of(0, 0)] = orbital[0]
    for n, chunk in enumerate(prepared_kernel(kernel[...], flips, row_flip[...], edge)):
        spectrum[n] = chunk
    twiddle = twiddle_ref[...]
    edge_tab = edge_table[...]

    forwards = []
    for t, u in box_moves:
        slot = slot_of(t, u)
        pltpu.make_async_remote_copy(
            src_ref=orbital.at[0, share],
            dst_ref=boxes.at[slot, share],
            send_sem=box_send.at[slot],
            recv_sem=box_recv.at[slot],
            device_id=place({"slab": t, "orb": u}),
            device_id_type=MESH,
        ).wait_recv()
        for v in range(1, reps):
            copy = pltpu.make_async_remote_copy(
                src_ref=boxes.at[slot, share],
                dst_ref=boxes.at[slot, share],
                send_sem=fwd_send.at[slot, v],
                recv_sem=fwd_recv.at[slot, v],
                device_id=place({"rep": v}),
                device_id_type=MESH,
            )
            copy.start()
            forwards.append(copy)
    table_copy.wait()
    for copy in forwards:
        copy.wait()

    lengths = (G, G, ZDEV * slabs)
    lane = lax.broadcasted_iota(jnp.int32, (1, plane), 1)
    lane_b, lane_c = lane // edge, lane % edge
    row = lax.broadcasted_iota(jnp.int32, (edge, 1), 0)
    own_row = slab * orbs + orb

    def moved_box(number):
        partner = partners[0, number * reps + rep]
        known = jnp.maximum(partner, 0)
        offsets = []
        for axis, length in enumerate(lengths):
            delta = corners[own_row, axis] - corners[known, axis]
            delta = jnp.where(delta < -(length // 2), delta + length, delta)
            delta = jnp.where(delta >= length - length // 2, delta - length, delta)
            offsets.append(delta)
        along_a, along_b, along_c = offsets
        step = known // orbs - slab + shift_back + 2 * slabs
        turn = lax.rem(known % orbs - orb + orbs, orbs)
        slot = jnp.minimum(lax.rem(step, slabs) * orbs + turn, boxes.shape[0] - 1)
        box = boxes[slot].astype(jnp.float32)
        box = pltpu.roll(box, (2 * plane - along_b * edge - along_c) % plane, 1)
        box = pltpu.roll(box, (2 * edge - along_a) % edge, 0)
        from_a, from_b, from_c = row + along_a, lane_b + along_b, lane_c + along_c
        usable = jnp.where(partner >= 0, edge, 0)
        inside_a = (from_a >= 0) & (from_a < usable)
        inside = (from_b >= 0) & (from_b < edge) & (from_c >= 0) & (from_c < edge)
        return jnp.where(inside_a & inside, box, 0.0)

    part = plane // RADIX
    cuts = [slice(n * part, (n + 1) * part) for n in range(RADIX)]
    total = jnp.zeros((edge, plane), jnp.float32)
    for start in range(0, slot_count, 2 * FIELDS):
        moved = [moved_box(n) for n in range(start, min(start + 2 * FIELDS, slot_count))]
        if len(moved) % 2:
            moved.append(jnp.zeros((edge, plane), jnp.float32))
        blocks = []
        for n in range(0, len(moved), 2):
            re, im = centre * moved[n], centre * moved[n + 1]
            re, im = butterfly([re[:, c] for c in cuts], [im[:, c] for c in cuts])
            blocks += [twiddled(re[k], im[k], k, twiddle) for k in range(RADIX)]
        blocks = plane_turn(blocks, plane_table[...])
        for n, block in enumerate(blocks):
            re, im = edge_turn(block, edge_tab)
            factor = spectrum[n % RADIX]
            blocks[n] = edge_turn((re * factor, -im * factor), edge_tab)
        blocks = plane_turn(blocks, plane_table[...])
        for n in range(0, len(moved), 2):
            field = blocks[n // 2 * RADIX : (n // 2 + 1) * RADIX]
            field = [twiddled(re, im, k, twiddle) for k, (re, im) in enumerate(field)]
            re, im = butterfly([f[0] for f in field], [f[1] for f in field])
            re, im = jnp.concatenate(re, axis=1), jnp.concatenate(im, axis=1)
            total = total + (im * moved[n + 1] - re * moved[n])
    mine[0] = total
    weighed = centre * total
    tile = weighed[:, :128]
    for n in range(128, plane, 128):
        tile = tile + weighed[:, n : n + 128]
    tile = sum(tile[n : n + 8] for n in range(8, edge, 8)) + tile[:8]

    swaps = []
    for v in range(1, reps):
        copy = pltpu.make_async_remote_copy(
            src_ref=mine,
            dst_ref=theirs.at[pl.ds(v - 1, 1)],
            send_sem=out_send.at[v - 1],
            recv_sem=out_recv.at[v - 1],
            device_id=place({"rep": v}),
            device_id_type=MESH,
        )
        copy.start()
        swaps.append(copy)

    for stage, (axes, moves) in enumerate(zip(stages, stage_moves)):
        count = math.prod(sizes[a] for a in axes)

        def number(moved):
            result = 0
            for a in axes:
                result = result * sizes[a] + moved.get(a, here[a])
            return result

        me = number({})
        energies[stage, me] = tile
        copies = []
        for n, m in enumerate(moves):
            copies.append(
                pltpu.make_async_remote_copy(
                    src_ref=energies.at[stage, me],
                    dst_ref=energies.at[stage, me],
                    send_sem=energy_send.at[stage, n],
                    recv_sem=energy_recv.at[stage, n],
                    device_id=place(m),
                    device_id_type=MESH,
                )
            )
            copies[-1].start()
        for copy in copies:
            copy.wait()
        tile = energies[stage, 0]
        for n in range(1, count):
            tile = tile + energies[stage, n]
    orbital_total = slabs * orbs
    value = jnp.sum(tile, keepdims=True) * (1.0 / (2.0 * orbital_total * edge**3))
    energy_out[...] = jnp.broadcast_to(value, energy_out.shape)
    for copy in swaps:
        copy.wait()
    for _, copy in sends:
        copy.wait_send()


def body(orbitals, corners, partners, kernel):
    own_count, edge, plane = orbitals.shape
    assert own_count == 1
    slabs, orbs, reps = (lax.axis_size(a) for a in ("slab", "orb", "rep"))
    depth = (ZDEV + edge - 2) // ZDEV
    if slabs <= 2 * depth + 1:
        steps, shift_back = tuple(range(slabs)), 0
    else:
        steps, shift_back = tuple(range(-depth, depth + 1)), depth
    slot_count = -(-min(partners.shape[1], slabs * orbs) // reps)
    if slabs * orbs * reps <= 16:
        stages = (("slab", "orb", "rep"),)
    else:
        stages = (("orb", "rep"), ("slab",))
    sizes = {"slab": slabs, "orb": orbs, "rep": reps}
    widest = max(math.prod(sizes[a] for a in axes) for axes in stages)
    cfg = (slabs, orbs, reps, steps, shift_back, slot_count, stages)
    edge_stack, plane_stack, twiddle, flips, row_flip = tables(edge)
    count = len(steps) * orbs
    vmem = pl.BlockSpec(memory_space=pltpu.VMEM)
    smem = pl.BlockSpec(memory_space=pltpu.SMEM)
    dma = pltpu.SemaphoreType.DMA
    mine, theirs, energy = pl.pallas_call(
        functools.partial(fused, cfg),
        out_shape=(
            jax.ShapeDtypeStruct((1, edge, plane), jnp.float32),
            jax.ShapeDtypeStruct((max(reps - 1, 1), edge, plane), jnp.float32),
            jax.ShapeDtypeStruct((8, 128), jnp.float32),
        ),
        in_specs=[smem, smem, vmem, vmem, vmem, pl.BlockSpec(memory_space=pl.ANY), vmem, vmem, vmem],
        out_specs=(vmem, vmem, vmem),
        scratch_shapes=[
            pltpu.VMEM((count, edge, plane), jnp.bfloat16),
            pltpu.VMEM(plane_stack.shape, jnp.bfloat16),
            pltpu.VMEM((RADIX, edge, plane // RADIX), jnp.float32),
            pltpu.VMEM((len(stages), widest, 8, 128), jnp.float32),
            dma,
            dma((count,)),
            dma((count,)),
            dma((count, reps)),
            dma((count, reps)),
            dma((reps,)),
            dma((reps,)),
            dma((len(stages), widest)),
            dma((len(stages), widest)),
        ],
        compiler_params=pltpu.CompilerParams(collective_id=0, has_side_effects=True),
    )(
        partners,
        corners,
        orbitals,
        kernel,
        jnp.asarray(edge_stack),
        jnp.asarray(plane_stack),
        jnp.asarray(twiddle),
        jnp.asarray(flips),
        jnp.asarray(row_flip),
    )
    result = mine
    for v in range(reps - 1):
        result = result + theirs[v : v + 1]
    return result, energy[0, :1]


def solution(mesh):
    in_specs = (
        P(("grp", "slab", "orb"), None, None),
        P("grp", None),
        P(("grp", "slab", "orb"), None),
        P(),
    )
    out_specs = (P(("grp", "slab", "orb"), None, None), P("grp"))
    return jax.shard_map(body, mesh=mesh, in_specs=in_specs, out_specs=out_specs, check_vma=False)
```

```python
import functools
import math

import jax
import jax.numpy as jnp
import numpy as np
from jax import lax
from jax.experimental import pallas as pl
from jax.experimental.pallas import tpu as pltpu
from jax.sharding import PartitionSpec as P

G = 192
ZDEV = 12
RADIX = 4
FIELDS = 2
MESH = pl.DeviceIdType.MESH


def split_np(values):
    high = values.astype(jnp.bfloat16)
    low = (values - high.astype(np.float64)).astype(jnp.bfloat16)
    return high, low


@functools.lru_cache(None)
def tables(edge):
    inner = edge // RADIX
    part = inner * edge
    turn = 2.0 * math.pi / edge
    ids = np.arange(edge)
    angles = (ids[:, None] * ids[None, :] % edge) * turn
    cosine, sine = np.cos(angles), np.sin(angles)
    edge_table = np.block([[cosine, sine], [-sine, cosine]])
    high, low = split_np(edge_table)
    edge_stack = np.concatenate([high, high, low], axis=1)
    lanes = np.arange(part)
    lane_b, lane_c = lanes // edge, lanes % edge
    phases = (RADIX * lane_b[:, None] * lane_b[None, :] + lane_c[:, None] * lane_c[None, :]) % edge
    cosine, sine = np.cos(phases * turn), np.sin(phases * turn)
    blocks = []
    for half in (np.concatenate([cosine, -sine], axis=1), np.concatenate([sine, cosine], axis=1)):
        high, low = split_np(half)
        blocks += [high, high, low]
    plane_stack = np.concatenate(blocks, axis=0)
    twiddle = []
    for first in range(RADIX):
        phase = (lane_b * first % edge) * turn
        twiddle += [np.cos(phase), np.sin(phase)]
    twiddle = np.stack(twiddle).astype(np.float32)
    flips = []
    for outer in (-lane_b % inner, inner - 1 - lane_b):
        source = outer * edge + (-lane_c % edge)
        flips.append((lanes[:, None] == source[None, :]).astype(jnp.bfloat16))
    flips = np.stack(flips)
    rows = (ids[:, None] == (-ids % edge)[None, :]).astype(jnp.bfloat16)
    row_flip = np.concatenate([rows, rows], axis=1)
    return edge_stack, plane_stack, twiddle, flips, row_flip


def parts(values):
    high = values.astype(jnp.bfloat16)
    return high, (values - high.astype(jnp.float32)).astype(jnp.bfloat16)


def dot(left, right):
    return jnp.dot(left, right, preferred_element_type=jnp.float32)


def butterfly(re, im):
    sum_re, sum_im = re[0] + re[2], im[0] + im[2]
    dif_re, dif_im = re[0] - re[2], im[0] - im[2]
    odd_re, odd_im = re[1] + re[3], im[1] + im[3]
    gap_re, gap_im = re[1] - re[3], im[1] - im[3]
    return (
        [sum_re + odd_re, dif_re + gap_im, sum_re - odd_re, dif_re - gap_im],
        [sum_im + odd_im, dif_im - gap_re, sum_im - odd_im, dif_im + gap_re],
    )


def twiddled(re, im, first, twiddle):
    if first == 0:
        return re, im
    cosine, sine = twiddle[2 * first : 2 * first + 1], twiddle[2 * first + 1 : 2 * first + 2]
    return re * cosine + im * sine, im * cosine - re * sine


def plane_turn(blocks, plane_table):
    rows = []
    for re, im in blocks:
        re_high, re_low = parts(re)
        im_high, im_low = parts(im)
        rows.append(
            jnp.concatenate([re_high, re_low, re_high, im_high, im_low, im_high], axis=1)
        )
    result = dot(jnp.concatenate(rows, axis=0), plane_table)
    edge, part = blocks[0][0].shape
    return [
        (result[n * edge : (n + 1) * edge, :part], result[n * edge : (n + 1) * edge, part:])
        for n in range(len(blocks))
    ]


def edge_turn(block, edge_table):
    re, im = block
    edge = re.shape[0]
    re_high, re_low = parts(re)
    im_high, im_low = parts(im)
    column = jnp.concatenate([re_high, im_high, re_low, im_low, re_high, im_high], axis=0)
    result = dot(edge_table, column)
    return result[:edge], result[edge:]


def prepared_kernel(values, flips, row_flip, edge):
    inner = edge // RADIX
    part = inner * edge
    width = RADIX * edge
    segment = lax.broadcasted_iota(jnp.int32, (edge, width), 1) // edge
    chunks = []
    for first in range(RADIX):
        pieces = []
        for group in range(part // width):
            piece = None
            for place in range(RADIX):
                source = RADIX * group + place
                moved = values[:, source * width : (source + 1) * width]
                shift = (place - first) * edge % width
                if shift:
                    moved = pltpu.roll(moved, shift, 1)
                piece = moved if piece is None else jnp.where(segment == place, moved, piece)
            pieces.append(piece)
        chunks.append(jnp.concatenate(pieces, axis=1))
    scale = 0.5 / float(edge**3)
    result = []
    for first in range(RADIX):
        high, low = parts(chunks[-first % RADIX])
        flip = flips[0] if first == 0 else flips[1]
        swapped = dot(jnp.concatenate([high, low], axis=0), flip).astype(jnp.bfloat16)
        result.append((chunks[first] + dot(row_flip, swapped)) * scale)
    return result


def fused(
    cfg,
    *refs,
):
    (
        partners_hbm,
        corners_hbm,
        orbital_hbm,
        kernel_hbm,
        edge_hbm,
        plane_hbm,
        twiddle_hbm,
        flips_hbm,
        row_hbm,
        mine,
        theirs,
        energy_out,
        partners,
        corners,
        orbital,
        kernel,
        edge_table,
        twiddle_ref,
        flips,
        row_flip,
        boxes,
        plane_table,
        spectrum,
        energies,
        load_sem,
        box_send,
        box_recv,
        fwd_send,
        fwd_recv,
        out_send,
        out_recv,
        energy_send,
        energy_recv,
    ) = refs
    slabs, orbs, reps, steps, shift_back, slot_count, stages = cfg
    edge, plane = orbital.shape[1], orbital.shape[2]
    slab, orb, rep = lax.axis_index("slab"), lax.axis_index("orb"), lax.axis_index("rep")
    sizes = {"slab": slabs, "orb": orbs, "rep": reps}
    here = {"slab": slab, "orb": orb, "rep": rep}

    def place(moves):
        return {a: lax.rem(here[a] + moves[a] % sizes[a], sizes[a]) for a in moves}

    box_moves = [(t, u) for t in steps for u in range(orbs) if (t % slabs, u) != (0, 0)]
    reached = {(t % slabs, u, 0) for t, u in box_moves} | {(0, 0, v) for v in range(1, reps)}
    stage_moves = []
    for axes in stages:
        moves = [{}]
        for a in axes:
            moves = [dict(m, **{a: n}) for m in moves for n in range(sizes[a])]
        stage_moves.append([m for m in moves if any(m.values())])
        reached |= {(m.get("slab", 0), m.get("orb", 0), m.get("rep", 0)) for m in stage_moves[-1]}
    reached |= {(-t % slabs, -u % orbs, -v % reps) for t, u, v in reached}
    reached = sorted(reached)

    loads = [
        pltpu.make_async_copy(source, target, load_sem.at[n])
        for n, (source, target) in enumerate(
            [
                (orbital_hbm, orbital),
                (kernel_hbm, kernel),
                (flips_hbm, flips),
                (row_hbm, row_flip),
                (partners_hbm, partners),
                (corners_hbm, corners),
                (twiddle_hbm, twiddle_ref),
                (edge_hbm, edge_table),
                (plane_hbm, plane_table),
            ]
        )
    ]
    for load in loads:
        load.start()
    barrier = pltpu.get_barrier_semaphore()
    for t, u, v in reached:
        pl.semaphore_signal(
            barrier,
            inc=1,
            device_id=place({"slab": t, "orb": u, "rep": v}),
            device_id_type=MESH,
        )
    loads[0].wait()
    pl.semaphore_wait(barrier, len(reached))

    def slot_of(t, u):
        return (t + shift_back) % slabs * orbs + u % orbs

    cut = edge // reps
    share = pl.ds(pl.multiple_of(rep * cut, cut), cut)
    sends = []
    for t, u in box_moves:
        target = slot_of(-t, -u)
        copy = pltpu.make_async_remote_copy(
            src_ref=orbital.at[0, share],
            dst_ref=boxes.at[target, share],
            send_sem=box_send.at[target],
            recv_sem=box_recv.at[target],
            device_id=place({"slab": t, "orb": u}),
            device_id_type=MESH,
        )
        copy.start()
        sends.append((slot_of(t, u), copy))

    centre = orbital[0].astype(jnp.float32)
    boxes[slot_of(0, 0)] = orbital[0]
    for load in loads[1:4]:
        load.wait()
    for n, chunk in enumerate(prepared_kernel(kernel[...], flips, row_flip[...], edge)):
        spectrum[n] = chunk

    forwards = []
    for t, u in box_moves:
        slot = slot_of(t, u)
        pltpu.make_async_remote_copy(
            src_ref=orbital.at[0, share],
            dst_ref=boxes.at[slot, share],
            send_sem=box_send.at[slot],
            recv_sem=box_recv.at[slot],
            device_id=place({"slab": t, "orb": u}),
            device_id_type=MESH,
        ).wait_recv()
        for v in range(1, reps):
            copy = pltpu.make_async_remote_copy(
                src_ref=boxes.at[slot, share],
                dst_ref=boxes.at[slot, share],
                send_sem=fwd_send.at[slot, v],
                recv_sem=fwd_recv.at[slot, v],
                device_id=place({"rep": v}),
                device_id_type=MESH,
            )
            copy.start()
            forwards.append(copy)
    for load in loads[4:]:
        load.wait()
    twiddle = twiddle_ref[...]
    edge_tab = edge_table[...]
    for copy in forwards:
        copy.wait()

    lengths = (G, G, ZDEV * slabs)
    lane = lax.broadcasted_iota(jnp.int32, (1, plane), 1)
    lane_b, lane_c = lane // edge, lane % edge
    row = lax.broadcasted_iota(jnp.int32, (edge, 1), 0)
    own_row = slab * orbs + orb

    def moved_box(number):
        partner = partners[0, number * reps + rep]
        known = jnp.maximum(partner, 0)
        offsets = []
        for axis, length in enumerate(lengths):
            delta = corners[axis, own_row] - corners[axis, known]
            delta = jnp.where(delta < -(length // 2), delta + length, delta)
            delta = jnp.where(delta >= length - length // 2, delta - length, delta)
            offsets.append(delta)
        along_a, along_b, along_c = offsets
        step = known // orbs - slab + shift_back + 2 * slabs
        turn = lax.rem(known % orbs - orb + orbs, orbs)
        slot = jnp.minimum(lax.rem(step, slabs) * orbs + turn, boxes.shape[0] - 1)
        box = boxes[slot].astype(jnp.float32)
        box = pltpu.roll(box, (2 * plane - along_b * edge - along_c) % plane, 1)
        box = pltpu.roll(box, (2 * edge - along_a) % edge, 0)
        from_a, from_b, from_c = row + along_a, lane_b + along_b, lane_c + along_c
        usable = jnp.where(partner >= 0, edge, 0)
        inside_a = (from_a >= 0) & (from_a < usable)
        inside = (from_b >= 0) & (from_b < edge) & (from_c >= 0) & (from_c < edge)
        return jnp.where(inside_a & inside, box, 0.0)

    def start_stage(stage, tile):
        me = number_of(stage, {})
        energies[stage, me] = tile
        copies = []
        for n, m in enumerate(stage_moves[stage]):
            copies.append(
                pltpu.make_async_remote_copy(
                    src_ref=energies.at[stage, me],
                    dst_ref=energies.at[stage, me],
                    send_sem=energy_send.at[stage, n],
                    recv_sem=energy_recv.at[stage, n],
                    device_id=place(m),
                    device_id_type=MESH,
                )
            )
            copies[-1].start()
        return copies

    def finish_stage(stage, copies):
        for copy in copies:
            copy.wait()
        result = energies[stage, 0]
        for n in range(1, math.prod(sizes[a] for a in stages[stage])):
            result = result + energies[stage, n]
        return result

    def number_of(stage, moved):
        result = 0
        for a in stages[stage]:
            result = result * sizes[a] + moved.get(a, here[a])
        return result

    part = plane // RADIX
    weighed = jnp.zeros((edge, part), jnp.float32)
    cuts = [slice(n * part, (n + 1) * part) for n in range(RADIX)]
    total = jnp.zeros((edge, plane), jnp.float32)
    for start in range(0, slot_count, 2 * FIELDS):
        moved = [moved_box(n) for n in range(start, min(start + 2 * FIELDS, slot_count))]
        if len(moved) % 2:
            moved.append(jnp.zeros((edge, plane), jnp.float32))
        blocks = []
        for n in range(0, len(moved), 2):
            re, im = centre * moved[n], centre * moved[n + 1]
            re, im = butterfly([re[:, c] for c in cuts], [im[:, c] for c in cuts])
            blocks += [twiddled(re[k], im[k], k, twiddle) for k in range(RADIX)]
        blocks = plane_turn(blocks, plane_table[...])
        for n, block in enumerate(blocks):
            re, im = edge_turn(block, edge_tab)
            factor = spectrum[n % RADIX]
            blocks[n] = (re * factor, -im * factor)
            weighed = weighed + (re * blocks[n][0] - im * blocks[n][1])
        if start + 2 * FIELDS >= slot_count:
            tile = weighed[:, :128]
            for n in range(128, part, 128):
                tile = tile + weighed[:, n : n + 128]
            tile = sum(tile[n : n + 8] for n in range(8, edge, 8)) + tile[:8]
            copies = start_stage(0, tile)
        blocks = [edge_turn(block, edge_tab) for block in blocks]
        blocks = plane_turn(blocks, plane_table[...])
        for n in range(0, len(moved), 2):
            field = blocks[n // 2 * RADIX : (n // 2 + 1) * RADIX]
            field = [twiddled(re, im, k, twiddle) for k, (re, im) in enumerate(field)]
            re, im = butterfly([f[0] for f in field], [f[1] for f in field])
            re, im = jnp.concatenate(re, axis=1), jnp.concatenate(im, axis=1)
            total = total + (im * moved[n + 1] - re * moved[n])
    mine[0] = total
    swaps = []
    for v in range(1, reps):
        copy = pltpu.make_async_remote_copy(
            src_ref=mine,
            dst_ref=theirs.at[pl.ds(v - 1, 1)],
            send_sem=out_send.at[v - 1],
            recv_sem=out_recv.at[v - 1],
            device_id=place({"rep": v}),
            device_id_type=MESH,
        )
        copy.start()
        swaps.append(copy)

    tile = finish_stage(0, copies)
    for stage in range(1, len(stages)):
        tile = finish_stage(stage, start_stage(stage, tile))
    energy_out[...] = tile
    for copy in swaps:
        copy.wait()
    for _, copy in sends:
        copy.wait_send()


def finished(scale, reps, mine, theirs, energy, result, total):
    value = mine[0]
    for v in range(reps - 1):
        value = value + theirs[v]
    result[0] = value
    total[0] = jnp.sum(energy[...]) * scale


def body(orbitals, corners, partners, kernel):
    own_count, edge, plane = orbitals.shape
    assert own_count == 1
    slabs, orbs, reps = (lax.axis_size(a) for a in ("slab", "orb", "rep"))
    depth = (ZDEV + edge - 2) // ZDEV
    if slabs <= 2 * depth + 1:
        steps, shift_back = tuple(range(slabs)), 0
    else:
        steps, shift_back = tuple(range(-depth, depth + 1)), depth
    slot_count = -(-min(partners.shape[1], slabs * orbs) // reps)
    if slabs * orbs * reps <= 16:
        stages = (("slab", "orb", "rep"),)
    else:
        stages = (("orb", "rep"), ("slab",))
    sizes = {"slab": slabs, "orb": orbs, "rep": reps}
    widest = max(math.prod(sizes[a] for a in axes) for axes in stages)
    cfg = (slabs, orbs, reps, steps, shift_back, slot_count, stages)
    edge_stack, plane_stack, twiddle, flips, row_flip = tables(edge)
    count = len(steps) * orbs
    vmem = pl.BlockSpec(memory_space=pltpu.VMEM)
    dma = pltpu.SemaphoreType.DMA
    mine, theirs, energy = pl.pallas_call(
        functools.partial(fused, cfg),
        out_shape=(
            jax.ShapeDtypeStruct((1, edge, plane), jnp.float32),
            jax.ShapeDtypeStruct((max(reps - 1, 1), edge, plane), jnp.float32),
            jax.ShapeDtypeStruct((8, 128), jnp.float32),
        ),
        in_specs=[pl.BlockSpec(memory_space=pl.ANY)] * 9,
        out_specs=(vmem, vmem, vmem),
        scratch_shapes=[
            pltpu.SMEM(partners.shape, jnp.int32),
            pltpu.SMEM(corners.shape[::-1], jnp.int32),
            pltpu.VMEM(orbitals.shape, jnp.bfloat16),
            pltpu.VMEM(kernel.shape, jnp.float32),
            pltpu.VMEM(edge_stack.shape, jnp.bfloat16),
            pltpu.VMEM(twiddle.shape, jnp.float32),
            pltpu.VMEM(flips.shape, jnp.bfloat16),
            pltpu.VMEM(row_flip.shape, jnp.bfloat16),
            pltpu.VMEM((count, edge, plane), jnp.bfloat16),
            pltpu.VMEM(plane_stack.shape, jnp.bfloat16),
            pltpu.VMEM((RADIX, edge, plane // RADIX), jnp.float32),
            pltpu.VMEM((len(stages), widest, 8, 128), jnp.float32),
            dma((9,)),
            dma((count,)),
            dma((count,)),
            dma((count, reps)),
            dma((count, reps)),
            dma((reps,)),
            dma((reps,)),
            dma((len(stages), widest)),
            dma((len(stages), widest)),
        ],
        compiler_params=pltpu.CompilerParams(collective_id=0, has_side_effects=True),
    )(
        partners,
        corners.T,
        orbitals,
        kernel,
        jnp.asarray(edge_stack),
        jnp.asarray(plane_stack),
        jnp.asarray(twiddle),
        jnp.asarray(flips),
        jnp.asarray(row_flip),
    )
    scale = -1.0 / (2.0 * slabs * orbs * edge**3)
    return pl.pallas_call(
        functools.partial(finished, scale, reps),
        out_shape=(
            jax.ShapeDtypeStruct((1, edge, plane), jnp.float32),
            jax.ShapeDtypeStruct((1,), jnp.float32),
        ),
        in_specs=[vmem] * 3,
        out_specs=(vmem, pl.BlockSpec(memory_space=pltpu.SMEM)),
    )(mine, theirs, energy)


def solution(mesh):
    in_specs = (
        P(("grp", "slab", "orb"), None, None),
        P("grp", None),
        P(("grp", "slab", "orb"), None),
        P(),
    )
    out_specs = (P(("grp", "slab", "orb"), None, None), P("grp"))
    return jax.shard_map(body, mesh=mesh, in_specs=in_specs, out_specs=out_specs, check_vma=False)
```

```python
import functools
import math

import jax
import jax.numpy as jnp
import numpy as np
from jax import lax
from jax.experimental import pallas as pl
from jax.experimental.pallas import tpu as pltpu
from jax.sharding import PartitionSpec as P

G = 192
ZDEV = 12
RADIX = 4
FIELDS = 2
MESH = pl.DeviceIdType.MESH


def split_np(values):
    high = values.astype(jnp.bfloat16)
    low = (values - high.astype(np.float64)).astype(jnp.bfloat16)
    return high, low


@functools.lru_cache(None)
def tables(edge):
    inner = edge // RADIX
    part = inner * edge
    turn = 2.0 * math.pi / edge
    ids = np.arange(edge)
    angles = (ids[:, None] * ids[None, :] % edge) * turn
    cosine, sine = np.cos(angles), np.sin(angles)
    edge_table = np.block([[cosine, sine], [-sine, cosine]])
    high, low = split_np(edge_table)
    edge_stack = np.concatenate([high, high, low], axis=1)
    lanes = np.arange(part)
    lane_b, lane_c = lanes // edge, lanes % edge
    phases = (RADIX * lane_b[:, None] * lane_b[None, :] + lane_c[:, None] * lane_c[None, :]) % edge
    cosine, sine = np.cos(phases * turn), np.sin(phases * turn)
    blocks = []
    for half in (np.concatenate([cosine, -sine], axis=1), np.concatenate([sine, cosine], axis=1)):
        high, low = split_np(half)
        blocks += [high, high, low]
    plane_stack = np.concatenate(blocks, axis=0)
    twiddle = []
    for first in range(RADIX):
        phase = (lane_b * first % edge) * turn
        twiddle += [np.cos(phase), np.sin(phase)]
    twiddle = np.stack(twiddle).astype(np.float32)
    flips = []
    for outer in (-lane_b % inner, inner - 1 - lane_b):
        source = outer * edge + (-lane_c % edge)
        flips.append((lanes[:, None] == source[None, :]).astype(jnp.bfloat16))
    flips = np.stack(flips)
    rows = (ids[:, None] == (-ids % edge)[None, :]).astype(jnp.bfloat16)
    row_flip = np.concatenate([rows, rows], axis=1)
    return edge_stack, plane_stack, twiddle, flips, row_flip


def parts(values):
    high = values.astype(jnp.bfloat16)
    return high, (values - high.astype(jnp.float32)).astype(jnp.bfloat16)


def dot(left, right):
    return jnp.dot(left, right, preferred_element_type=jnp.float32)


def butterfly(re, im):
    sum_re, sum_im = re[0] + re[2], im[0] + im[2]
    dif_re, dif_im = re[0] - re[2], im[0] - im[2]
    odd_re, odd_im = re[1] + re[3], im[1] + im[3]
    gap_re, gap_im = re[1] - re[3], im[1] - im[3]
    return (
        [sum_re + odd_re, dif_re + gap_im, sum_re - odd_re, dif_re - gap_im],
        [sum_im + odd_im, dif_im - gap_re, sum_im - odd_im, dif_im + gap_re],
    )


def twiddled(re, im, first, twiddle):
    if first == 0:
        return re, im
    cosine, sine = twiddle[2 * first : 2 * first + 1], twiddle[2 * first + 1 : 2 * first + 2]
    return re * cosine + im * sine, im * cosine - re * sine


def plane_turn(blocks, plane_table):
    rows = []
    for re, im in blocks:
        re_high, re_low = parts(re)
        im_high, im_low = parts(im)
        rows.append(
            jnp.concatenate([re_high, re_low, re_high, im_high, im_low, im_high], axis=1)
        )
    result = dot(jnp.concatenate(rows, axis=0), plane_table)
    edge, part = blocks[0][0].shape
    return [
        (result[n * edge : (n + 1) * edge, :part], result[n * edge : (n + 1) * edge, part:])
        for n in range(len(blocks))
    ]


def edge_turn(block, edge_table):
    re, im = block
    edge = re.shape[0]
    re_high, re_low = parts(re)
    im_high, im_low = parts(im)
    column = jnp.concatenate([re_high, im_high, re_low, im_low, re_high, im_high], axis=0)
    result = dot(edge_table, column)
    return result[:edge], result[edge:]


def prepared_kernel(values, flips, row_flip, edge):
    inner = edge // RADIX
    part = inner * edge
    width = RADIX * edge
    segment = lax.broadcasted_iota(jnp.int32, (edge, width), 1) // edge
    chunks = []
    for first in range(RADIX):
        pieces = []
        for group in range(part // width):
            piece = None
            for place in range(RADIX):
                source = RADIX * group + place
                moved = values[:, source * width : (source + 1) * width]
                shift = (place - first) * edge % width
                if shift:
                    moved = pltpu.roll(moved, shift, 1)
                piece = moved if piece is None else jnp.where(segment == place, moved, piece)
            pieces.append(piece)
        chunks.append(jnp.concatenate(pieces, axis=1))
    scale = 0.5 / float(edge**3)
    result = []
    for first in range(RADIX):
        high, low = parts(chunks[-first % RADIX])
        flip = flips[0] if first == 0 else flips[1]
        swapped = dot(jnp.concatenate([high, low], axis=0), flip).astype(jnp.bfloat16)
        result.append((chunks[first] + dot(row_flip, swapped)) * scale)
    return result


def fused(
    cfg,
    *refs,
):
    (
        partners_hbm,
        corners_hbm,
        orbital_hbm,
        kernel_hbm,
        edge_hbm,
        plane_hbm,
        twiddle_hbm,
        flips_hbm,
        row_hbm,
        mine,
        theirs,
        energy_out,
        partners,
        corners,
        orbital,
        kernel,
        edge_table,
        twiddle_ref,
        flips,
        row_flip,
        boxes,
        plane_table,
        spectrum,
        energies,
        load_sem,
        box_send,
        box_recv,
        fwd_send,
        fwd_recv,
        out_send,
        out_recv,
        energy_send,
        energy_recv,
    ) = refs
    slabs, orbs, reps, steps, shift_back, slot_count, stages = cfg
    edge, plane = orbital.shape[1], orbital.shape[2]
    slab, orb, rep = lax.axis_index("slab"), lax.axis_index("orb"), lax.axis_index("rep")
    sizes = {"slab": slabs, "orb": orbs, "rep": reps}
    here = {"slab": slab, "orb": orb, "rep": rep}

    def place(moves):
        return {a: lax.rem(here[a] + moves[a] % sizes[a], sizes[a]) for a in moves}

    box_moves = [(t, u) for t in steps for u in range(orbs) if (t % slabs, u) != (0, 0)]
    reached = {(t % slabs, u, 0) for t, u in box_moves} | {(0, 0, v) for v in range(1, reps)}
    stage_moves = []
    for axes in stages:
        moves = [{}]
        for a in axes:
            moves = [dict(m, **{a: n}) for m in moves for n in range(sizes[a])]
        stage_moves.append([m for m in moves if any(m.values())])
        reached |= {(m.get("slab", 0), m.get("orb", 0), m.get("rep", 0)) for m in stage_moves[-1]}
    reached |= {(-t % slabs, -u % orbs, -v % reps) for t, u, v in reached}
    reached = sorted(reached)

    loads = [
        pltpu.make_async_copy(source, target, load_sem.at[n])
        for n, (source, target) in enumerate(
            [
                (orbital_hbm, orbital),
                (kernel_hbm, kernel),
                (flips_hbm, flips),
                (row_hbm, row_flip),
                (partners_hbm, partners),
                (corners_hbm, corners),
                (twiddle_hbm, twiddle_ref),
                (edge_hbm, edge_table),
                (plane_hbm, plane_table),
            ]
        )
    ]
    for load in loads:
        load.start()
    barrier = pltpu.get_barrier_semaphore()
    for t, u, v in reached:
        pl.semaphore_signal(
            barrier,
            inc=1,
            device_id=place({"slab": t, "orb": u, "rep": v}),
            device_id_type=MESH,
        )
    loads[0].wait()
    pl.semaphore_wait(barrier, len(reached))

    def slot_of(t, u):
        return (t + shift_back) % slabs * orbs + u % orbs

    cut = edge // reps
    share = pl.ds(pl.multiple_of(rep * cut, cut), cut)
    sends = []

    def send(source, target, send_sem, move):
        copy = pltpu.make_async_remote_copy(
            src_ref=orbital.at[0, share] if source is None else boxes.at[source, share],
            dst_ref=boxes.at[target, share],
            send_sem=send_sem,
            recv_sem=box_recv.at[target],
            device_id=move,
            device_id_type=MESH,
        )
        copy.start()
        sends.append(copy)

    low = slab < slabs // 2
    moves = [t for t in steps if t % slabs]
    ordered = [
        jnp.where(low, after, before) if shift_back == 0 else after
        for before, after in zip(moves, reversed(moves))
    ]

    def slot_at(t, u=0):
        return lax.rem(t + shift_back + slabs, slabs) * orbs + u % orbs

    for u in range(1, orbs):
        send(None, slot_of(0, -u), box_send.at[slot_of(0, -u)], place({"orb": u}))
    for t in ordered:
        target = slot_at(-t)
        send(None, target, box_send.at[target], {"slab": lax.rem(slab + t + slabs, slabs)})

    centre = orbital[0].astype(jnp.float32)
    boxes[slot_of(0, 0)] = orbital[0]
    for load in loads[1:4]:
        load.wait()
    for n, chunk in enumerate(prepared_kernel(kernel[...], flips, row_flip[...], edge)):
        spectrum[n] = chunk

    forwards = []

    def arrived(slot):
        pltpu.make_async_remote_copy(
            src_ref=orbital.at[0, share],
            dst_ref=boxes.at[slot, share],
            send_sem=box_send.at[slot],
            recv_sem=box_recv.at[slot],
            device_id=place({"rep": 1}),
            device_id_type=MESH,
        ).wait_recv()

    def share_box(slot):
        for v in range(1, reps):
            copy = pltpu.make_async_remote_copy(
                src_ref=boxes.at[slot, share],
                dst_ref=boxes.at[slot, share],
                send_sem=fwd_send.at[slot, v],
                recv_sem=fwd_recv.at[slot, v],
                device_id=place({"rep": v}),
                device_id_type=MESH,
            )
            copy.start()
            forwards.append(copy)

    for t in reversed(ordered):
        arrived(slot_at(t))
        for u in range(1, orbs):
            target = slot_at(t, -u)
            send(slot_at(t), target, box_send.at[target], place({"orb": u}))
        share_box(slot_at(t))
    for u in range(1, orbs):
        for slot in [slot_of(0, u), *[slot_at(t, u) for t in reversed(ordered)]]:
            arrived(slot)
            share_box(slot)
    for load in loads[4:]:
        load.wait()
    twiddle = twiddle_ref[...]
    edge_tab = edge_table[...]
    for copy in forwards:
        copy.wait()

    lengths = (G, G, ZDEV * slabs)
    lane = lax.broadcasted_iota(jnp.int32, (1, plane), 1)
    lane_b, lane_c = lane // edge, lane % edge
    row = lax.broadcasted_iota(jnp.int32, (edge, 1), 0)
    own_row = slab * orbs + orb

    def moved_box(number):
        partner = partners[0, number * reps + rep]
        known = jnp.maximum(partner, 0)
        offsets = []
        for axis, length in enumerate(lengths):
            delta = corners[axis, own_row] - corners[axis, known]
            delta = jnp.where(delta < -(length // 2), delta + length, delta)
            delta = jnp.where(delta >= length - length // 2, delta - length, delta)
            offsets.append(delta)
        along_a, along_b, along_c = offsets
        step = known // orbs - slab + shift_back + 2 * slabs
        turn = lax.rem(known % orbs - orb + orbs, orbs)
        slot = jnp.minimum(lax.rem(step, slabs) * orbs + turn, boxes.shape[0] - 1)
        box = boxes[slot].astype(jnp.float32)
        box = pltpu.roll(box, (2 * plane - along_b * edge - along_c) % plane, 1)
        box = pltpu.roll(box, (2 * edge - along_a) % edge, 0)
        from_a, from_b, from_c = row + along_a, lane_b + along_b, lane_c + along_c
        usable = jnp.where(partner >= 0, edge, 0)
        inside_a = (from_a >= 0) & (from_a < usable)
        inside = (from_b >= 0) & (from_b < edge) & (from_c >= 0) & (from_c < edge)
        return jnp.where(inside_a & inside, box, 0.0)

    def start_stage(stage, tile):
        me = number_of(stage, {})
        energies[stage, me] = tile
        copies = []
        for n, m in enumerate(stage_moves[stage]):
            copies.append(
                pltpu.make_async_remote_copy(
                    src_ref=energies.at[stage, me],
                    dst_ref=energies.at[stage, me],
                    send_sem=energy_send.at[stage, n],
                    recv_sem=energy_recv.at[stage, n],
                    device_id=place(m),
                    device_id_type=MESH,
                )
            )
            copies[-1].start()
        return copies

    def finish_stage(stage, copies):
        for copy in copies:
            copy.wait()
        result = energies[stage, 0]
        for n in range(1, math.prod(sizes[a] for a in stages[stage])):
            result = result + energies[stage, n]
        return result

    def number_of(stage, moved):
        result = 0
        for a in stages[stage]:
            result = result * sizes[a] + moved.get(a, here[a])
        return result

    part = plane // RADIX
    weighed = jnp.zeros((edge, part), jnp.float32)
    cuts = [slice(n * part, (n + 1) * part) for n in range(RADIX)]
    total = jnp.zeros((edge, plane), jnp.float32)
    for start in range(0, slot_count, 2 * FIELDS):
        moved = [moved_box(n) for n in range(start, min(start + 2 * FIELDS, slot_count))]
        if len(moved) % 2:
            moved.append(jnp.zeros((edge, plane), jnp.float32))
        blocks = []
        for n in range(0, len(moved), 2):
            re, im = centre * moved[n], centre * moved[n + 1]
            re, im = butterfly([re[:, c] for c in cuts], [im[:, c] for c in cuts])
            blocks += [twiddled(re[k], im[k], k, twiddle) for k in range(RADIX)]
        blocks = plane_turn(blocks, plane_table[...])
        for n, block in enumerate(blocks):
            re, im = edge_turn(block, edge_tab)
            factor = spectrum[n % RADIX]
            blocks[n] = (re * factor, -im * factor)
            weighed = weighed + (re * blocks[n][0] - im * blocks[n][1])
        if start + 2 * FIELDS >= slot_count:
            tile = weighed[:, :128]
            for n in range(128, part, 128):
                tile = tile + weighed[:, n : n + 128]
            tile = sum(tile[n : n + 8] for n in range(8, edge, 8)) + tile[:8]
            copies = start_stage(0, tile)
        blocks = [edge_turn(block, edge_tab) for block in blocks]
        blocks = plane_turn(blocks, plane_table[...])
        for n in range(0, len(moved), 2):
            field = blocks[n // 2 * RADIX : (n // 2 + 1) * RADIX]
            field = [twiddled(re, im, k, twiddle) for k, (re, im) in enumerate(field)]
            re, im = butterfly([f[0] for f in field], [f[1] for f in field])
            re, im = jnp.concatenate(re, axis=1), jnp.concatenate(im, axis=1)
            total = total + (im * moved[n + 1] - re * moved[n])
    mine[0] = total
    swaps = []
    for v in range(1, reps):
        copy = pltpu.make_async_remote_copy(
            src_ref=mine,
            dst_ref=theirs.at[pl.ds(v - 1, 1)],
            send_sem=out_send.at[v - 1],
            recv_sem=out_recv.at[v - 1],
            device_id=place({"rep": v}),
            device_id_type=MESH,
        )
        copy.start()
        swaps.append(copy)

    tile = finish_stage(0, copies)
    for stage in range(1, len(stages)):
        tile = finish_stage(stage, start_stage(stage, tile))
    energy_out[...] = tile
    for copy in swaps:
        copy.wait()
    for copy in sends:
        copy.wait_send()


def finished(scale, reps, mine, theirs, energy, result, total):
    value = mine[0]
    for v in range(reps - 1):
        value = value + theirs[v]
    result[0] = value
    total[0] = jnp.sum(energy[...]) * scale


def body(orbitals, corners, partners, kernel):
    own_count, edge, plane = orbitals.shape
    assert own_count == 1
    slabs, orbs, reps = (lax.axis_size(a) for a in ("slab", "orb", "rep"))
    depth = (ZDEV + edge - 2) // ZDEV
    if slabs <= 2 * depth + 1:
        steps, shift_back = tuple(range(slabs)), 0
    else:
        steps, shift_back = tuple(range(-depth, depth + 1)), depth
    slot_count = -(-min(partners.shape[1], slabs * orbs) // reps)
    if slabs * orbs * reps <= 16:
        stages = (("slab", "orb", "rep"),)
    else:
        stages = (("orb", "rep"), ("slab",))
    sizes = {"slab": slabs, "orb": orbs, "rep": reps}
    widest = max(math.prod(sizes[a] for a in axes) for axes in stages)
    cfg = (slabs, orbs, reps, steps, shift_back, slot_count, stages)
    edge_stack, plane_stack, twiddle, flips, row_flip = tables(edge)
    count = len(steps) * orbs
    vmem = pl.BlockSpec(memory_space=pltpu.VMEM)
    dma = pltpu.SemaphoreType.DMA
    mine, theirs, energy = pl.pallas_call(
        functools.partial(fused, cfg),
        out_shape=(
            jax.ShapeDtypeStruct((1, edge, plane), jnp.float32),
            jax.ShapeDtypeStruct((max(reps - 1, 1), edge, plane), jnp.float32),
            jax.ShapeDtypeStruct((8, 128), jnp.float32),
        ),
        in_specs=[pl.BlockSpec(memory_space=pl.ANY)] * 9,
        out_specs=(vmem, vmem, vmem),
        scratch_shapes=[
            pltpu.SMEM(partners.shape, jnp.int32),
            pltpu.SMEM(corners.shape[::-1], jnp.int32),
            pltpu.VMEM(orbitals.shape, jnp.bfloat16),
            pltpu.VMEM(kernel.shape, jnp.float32),
            pltpu.VMEM(edge_stack.shape, jnp.bfloat16),
            pltpu.VMEM(twiddle.shape, jnp.float32),
            pltpu.VMEM(flips.shape, jnp.bfloat16),
            pltpu.VMEM(row_flip.shape, jnp.bfloat16),
            pltpu.VMEM((count, edge, plane), jnp.bfloat16),
            pltpu.VMEM(plane_stack.shape, jnp.bfloat16),
            pltpu.VMEM((RADIX, edge, plane // RADIX), jnp.float32),
            pltpu.VMEM((len(stages), widest, 8, 128), jnp.float32),
            dma((9,)),
            dma((count,)),
            dma((count,)),
            dma((count, reps)),
            dma((count, reps)),
            dma((reps,)),
            dma((reps,)),
            dma((len(stages), widest)),
            dma((len(stages), widest)),
        ],
        compiler_params=pltpu.CompilerParams(collective_id=0, has_side_effects=True),
    )(
        partners,
        corners.T,
        orbitals,
        kernel,
        jnp.asarray(edge_stack),
        jnp.asarray(plane_stack),
        jnp.asarray(twiddle),
        jnp.asarray(flips),
        jnp.asarray(row_flip),
    )
    scale = -1.0 / (2.0 * slabs * orbs * edge**3)
    return pl.pallas_call(
        functools.partial(finished, scale, reps),
        out_shape=(
            jax.ShapeDtypeStruct((1, edge, plane), jnp.float32),
            jax.ShapeDtypeStruct((1,), jnp.float32),
        ),
        in_specs=[vmem] * 3,
        out_specs=(vmem, pl.BlockSpec(memory_space=pltpu.SMEM)),
    )(mine, theirs, energy)


def solution(mesh):
    in_specs = (
        P(("grp", "slab", "orb"), None, None),
        P("grp", None),
        P(("grp", "slab", "orb"), None),
        P(),
    )
    out_specs = (P(("grp", "slab", "orb"), None, None), P("grp"))
    return jax.shard_map(body, mesh=mesh, in_specs=in_specs, out_specs=out_specs, check_vma=False)
```
